128 devices in a mesh: rows: 16 (over x, y_lo, core), dim: 8 (over y_hi, z).
Axes of the slice: x: 4, y: 4 (y_hi: 2, y_lo: 2; y = y_hi * 2 + y_lo), z: 4, core: 2. Of those that a mesh axis runs over, the one named last changes fastest.
Arguments:
- entity_table: float32 [524288, 512], P(('rows', 'dim')), may hold values from -2.5 to 2.5
- relations: float32 [822, 512], replicated, may hold values from -6 to 6
- thresholds: float32 [64], replicated, may hold values from 0.2 to 2
- head_ids: int32 [2048], replicated, may hold values from 0 to 524287
- rel_ids: int32 [2048], replicated, may hold values from 0 to 821
- thr_idx: int32 [2048], replicated, may hold values from 0 to 63
Outputs:
- serving_table: float32 [524288, 512], P('rows', 'dim')
- fraction: float32 [2048], P(('rows', 'dim'))
The draws below stay inside these ranges and needn't reach their ends.
All inputs are finite; a program needn't handle non-finite values.
Results may differ from the reference program's by a relative error of at most 0.0011.
Values sent between devices are 32-bit elements; how exact they have to be, the bound alone decides.
A program may use at most 128 MiB of HBM per device.

```python
import math
import jax
import jax.numpy as jnp
from jax import lax

D = 512
ENT_DEV = 4096
Q = 2048
NREL = 822
NTHR = 64
ENT = 524288


cluster_count = 32


def draw_entity_table(key, part):
    key_ids = jax.random.fold_in(key, 11)
    key_cent = jax.random.fold_in(key, 12)
    key_vals = jax.random.fold_in(key, 13)
    key_jit = jax.random.fold_in(key, 14)
    member = jax.random.randint(key_ids, (ENT,), 0, cluster_count)
    centers = jnp.clip(jax.random.normal(key_cent, (cluster_count, D), jnp.float32), -6.0, 6.0)
    shared = jnp.take(centers, member, axis=0)
    position = jnp.arange(ENT, dtype=jnp.float32)[:, None] / ENT
    jitter = jax.random.uniform(key_jit, (ENT, 1), jnp.float32, -0.5, 0.5)
    scale = float(D) ** (-0.25) * jnp.exp(math.log(3.0) * (position - 0.5) + jitter)
    noise = jnp.clip(jax.random.normal(key_vals, (ENT, D), jnp.float32), -6.0, 6.0)
    values = scale * (0.8 * shared + 0.6 * noise)
    return jnp.clip(values, -2.5, 2.5).astype(jnp.float32)


def place_ends(drawn, rng, least, top_value):
    spot = [jax.random.randint(jax.random.fold_in(rng, axis), (), 0, length) for axis, length in enumerate(drawn.shape)]
    widest = drawn.shape.index(max(drawn.shape))
    beside = spot[:widest] + [(spot[widest] + 1) % drawn.shape[widest]] + spot[widest + 1:]
    return drawn.at[tuple(spot)].set(least).at[tuple(beside)].set(top_value)


def scatter_about(stream_key, extent, deviation, reach, held_as=jnp.bfloat16):
    result = deviation * jax.random.normal(stream_key, extent, jnp.float32)
    return jnp.clip(result, min=-reach, max=reach).astype(held_as)


def setup_inputs(seed: int = 0) -> dict:
    key_of = jax.random.split(jax.random.key(seed), 7)
    return {
        "entity_table": draw_entity_table(jax.random.fold_in(key_of[6], 71), 0),
        "relations": scatter_about(key_of[1], (NREL, D), 1.0, 6.0, jnp.float32),
        "thresholds": jnp.clip(jax.random.uniform(key_of[2], (NTHR,), jnp.float32, 0.2, 2.0), 0.2, 2.0),
        "head_ids": place_ends(jax.random.randint(key_of[3], (Q,), 0, ENT), jax.random.fold_in(key_of[3], 1), 0, ENT - 1).astype(jnp.int32),
        "rel_ids": place_ends(jax.random.randint(key_of[4], (Q,), 0, NREL), jax.random.fold_in(key_of[4], 1), 0, NREL - 1).astype(jnp.int32),
        "thr_idx": place_ends(jax.random.randint(key_of[5], (Q,), 0, NTHR), jax.random.fold_in(key_of[5], 1), 0, NTHR - 1).astype(jnp.int32),
    }


sharpness = 2.0


def reference(entity_table, relations, thresholds, head_ids, rel_ids, thr_idx):
    head_vecs = jnp.take(entity_table, head_ids, axis=0)
    query = (head_vecs * jnp.take(relations, rel_ids, axis=0)).astype(jnp.bfloat16)
    query = lax.optimization_barrier(query).astype(jnp.float32)
    level = jnp.take(thresholds, thr_idx)
    block = ENT_DEV * 4
    count = ENT // block
    blocks = entity_table.reshape(count, block, D)

    def step(total, rows_block):
        ent_low = lax.optimization_barrier(rows_block.astype(jnp.bfloat16)).astype(jnp.float32)
        score = jnp.dot(query, ent_low.T, precision=lax.Precision.HIGHEST, preferred_element_type=jnp.float32)
        soft = jax.nn.sigmoid(sharpness * (score - level[:, None]))
        return total + jnp.sum(soft, axis=1), None

    total, unused = lax.scan(step, jnp.zeros((Q,), jnp.float32), blocks)
    return entity_table, total * (1.0 / ENT)
```

```python
import functools

import jax
import jax.numpy as jnp
from jax import lax
from jax.experimental import pallas as pl
from jax.experimental.pallas import tpu as pltpu
from jax.sharding import PartitionSpec as P

MESH = pl.DeviceIdType.MESH
F32 = jnp.float32
sharpness = 2.0

PLANE = [(a, b, z) for a in range(2) for b in range(2) for z in range(4)][1:]
SLABS = [(0, 0, 1), (0, 0, 3), (0, 1, 0), (0, 0, 2), (0, 1, 1), (0, 1, 3), (0, 1, 2)]
WAVES = [(0, 1152), (1152, 256), (1408, 1792), (3200, 896)]


def kernel(
    total_ents, head_ids, rel_ids, thresholds, table, relations, thr_idx,
    serving, share,
    tab, tab_t, ent, rel, theirs, mine, pair_in, x_in, plane_in, rel_rows, query_rows, queries,
    level, totals, pair_tot, x_tot, plane_tot,
    load_sem, own_sem, slab_send, slab_recv, pair_send, pair_recv, x_send, x_recv,
    plane_send, plane_recv, gath_send, gath_recv, xg_send, xg_recv, pg_send, pg_recv,
    tot_send, tot_recv,
):
    r, d = lax.axis_index("rows"), lax.axis_index("dim")
    x, y_lo, core = r // 4, (r // 2) % 2, r % 2
    y_hi, z = d // 4, d % 4
    ents = table.shape[0]
    width = table.shape[1]
    group = x_in.shape[1]
    slab = serving.shape[0]

    def at_plane(off):
        a, b, dz = off
        row = x * 4 + ((y_lo + a) % 2) * 2 + core
        return row, ((y_hi + b) % 2) * 4 + (z + dz) % 4

    def at_x(k):
        return ((x + k) % 4) * 4 + y_lo * 2 + core, d

    partner = (x * 4 + y_lo * 2 + (1 - core), d)

    def send(src, dst, s, t, peer):
        copy = pltpu.make_async_remote_copy(
            src_ref=src, dst_ref=dst, send_sem=s, recv_sem=t, device_id=peer, device_id_type=MESH
        )
        copy.start()
        return copy

    cuts = [0, WAVES[0][1], 2048, 3072, ents]
    loads = []
    for k in range(4):
        span = pl.ds(cuts[k], cuts[k + 1] - cuts[k])
        loads.append(pltpu.make_async_copy(table.at[span], tab.at[span], load_sem.at[k]))
        loads[-1].start()
    load_rel = pltpu.make_async_copy(relations, rel, load_sem.at[4])
    load_rel.start()
    barrier = pltpu.get_barrier_semaphore()
    peers = [at_plane(off) for off in PLANE] + [at_x(k) for k in (1, 2, 3)] + [partner]
    for peer in peers:
        pl.semaphore_signal(barrier, inc=1, device_id=peer, device_id_type=MESH)

    def transpose_rows(first, count):
        @pl.loop(0, count // 128)
        def _(i):
            span = pl.ds(pl.multiple_of(first + i * 128, 128), 128)
            tab_t[:, span] = tab[span, :].T

    slab_copies, own_copies = [], []

    def start_wave(w):
        first, count = WAVES[w]
        span = pl.ds(first, count)
        here = pl.ds(pl.multiple_of(d * ents + first, 128), count)
        for i, off in enumerate(SLABS):
            row, col = at_plane(off)
            rows = pl.ds(pl.multiple_of(col * slab, 8), slab)
            slab_copies.append(
                send(tab_t.at[rows, span], serving.at[:, here], slab_send.at[w, i], slab_recv.at[w, i], (row, col))
            )
        rows = pl.ds(pl.multiple_of(d * slab, 8), slab)
        own = pltpu.make_async_copy(tab_t.at[rows, span], serving.at[:, here], own_sem.at[w])
        own.start()
        own_copies.append(own)

    loads[0].wait()
    transpose_rows(*WAVES[0])
    pl.semaphore_wait(barrier, len(peers))
    start_wave(0)
    for k in range(1, 4):
        loads[k].wait()

    start = (r * lax.axis_size("dim") + d) * ents

    def pick(out, half):
        def part(k):
            @pl.loop(0, group // 8)
            def _(i):
                for j in range(8):
                    low = i * 8 + j
                    q = k * 512 + (low // 128) * 256 + half * 128 + low % 128
                    local = head_ids[q] - start
                    owned = jnp.logical_and(local >= 0, local < ents)
                    row = tab[pl.ds(jnp.clip(local, 0, ents - 1), 1), :]
                    out[k, pl.ds(low, 1), :] = jnp.where(owned, row, jnp.zeros_like(row))
        return part

    order = [(x + 2) % 4, (x + 1) % 4, (x + 3) % 4, x]
    copies = []
    for n in range(4):
        pick(theirs, 1 - core)(order[n])
        copies.append(send(theirs.at[order[n]], pair_in.at[order[n]], pair_send.at[n], pair_recv.at[n], partner))
    for n in range(4):
        pick(mine, core)(order[n])

    x_copies = {}
    for n, k in enumerate((2, 1, 3, 0)):
        copies[n].wait_recv()
        mine[order[n]] += pair_in[order[n]]
        if k:
            x_copies[k] = send(mine.at[order[n]], x_in.at[k - 1], x_send.at[k - 1], x_recv.at[k - 1], at_x(k))

    transpose_rows(WAVES[0][1], ents - WAVES[0][1])

    @pl.loop(0, ents // 256)
    def _(i):
        span = pl.ds(pl.multiple_of(i * 256, 256), 256)
        ent[span, :] = tab[span, :].astype(jnp.bfloat16)

    found = jnp.zeros(level.shape, F32)
    for k in range(thresholds.shape[0]):
        found = jnp.where(thr_idx[...] == k, thresholds[k], found)
    level[...] = found
    load_rel.wait()
    first_q = r * 128 + d * 16
    for i in range(16):
        rel_rows[pl.ds(i, 1), :] = rel[pl.ds(rel_ids[first_q + i], 1), :]

    for k in (1, 3, 2):
        x_copies[k].wait_recv()
        mine[x] += x_in[k - 1]

    def rows_of(row, col):
        return pl.ds(pl.multiple_of(((row // 2) % 2) * 128 + col * 16, 16), 16)

    plane_copies = []
    for i, off in enumerate(PLANE):
        peer = at_plane(off)
        plane_copies.append(
            send(mine.at[x, rows_of(*peer)], plane_in.at[i], plane_send.at[i], plane_recv.at[i], peer)
        )
    start_wave(1)
    head = mine[x, rows_of(r, d)]
    for i in range(15):
        plane_copies[i].wait_recv()
        head += plane_in[i]

    query_rows[...] = (head * rel_rows[...]).astype(jnp.bfloat16).astype(F32)
    own_group = core * 4 + x
    gath_copies = []
    for i, off in enumerate(PLANE):
        gath_copies.append(
            send(query_rows, queries.at[own_group, rows_of(r, d)], gath_send.at[i], gath_recv.at[i], at_plane(off))
        )
    start_wave(2)
    queries[own_group, rows_of(r, d)] = query_rows[...]
    for i in range(15):
        gath_copies[i].wait_recv()

    xg_copies = {}
    for k in (1, 3, 2):
        xg_copies[k] = send(queries.at[own_group], queries.at[own_group], xg_send.at[k - 1], xg_recv.at[k - 1], at_x(k))

    tile = 512

    def count(half, k):
        g = half * 4 + k
        low = queries[g].astype(jnp.bfloat16)
        lev = jnp.concatenate(
            [level[pl.ds(k * 4 + half, 1), :], level[pl.ds(k * 4 + 2 + half, 1), :]], axis=1
        )

        def step(i, acc):
            rows = ent[pl.ds(pl.multiple_of(i * tile, tile), tile), :]
            score = lax.dot_general(rows, low, (((1,), (1,)), ((), ())), preferred_element_type=F32)
            soft = 1.0 / (1.0 + jnp.exp(sharpness * (lev - score)))
            return acc + jnp.sum(soft.reshape(tile // 8, 8, group), axis=0)

        totals[g] = lax.fori_loop(0, ents // tile, step, jnp.zeros((8, group), F32))

    pg_copies = []
    for n, k in enumerate((0, 1, 3, 2)):
        from_x = (x + 4 - k) % 4
        if k:
            xg_copies[k].wait_recv()
        g = core * 4 + from_x
        pg_copies.append(send(queries.at[g], queries.at[g], pg_send.at[n], pg_recv.at[n], partner))
        count(core, from_x)
        pg_copies[n].wait_recv()
        count(1 - core, from_x)

    other = pl.ds((1 - core) * 4, 4)
    half = send(totals.at[other], pair_tot, tot_send.at[0], tot_recv.at[0], partner)
    half.wait_recv()
    x_tots = {}
    for k in (0, 1, 2, 3):
        to = (x + k) % 4
        x_tot[k] = totals[core * 4 + to] + pair_tot[to]
        if k:
            x_tots[k] = send(x_tot.at[k], x_tot.at[3 + k], tot_send.at[k], tot_recv.at[k], at_x(k))
    sums = x_tot[0]
    for k in (1, 2, 3):
        x_tots[k].wait_recv()
        sums += x_tot[3 + k]
    plane_tot[0] = sums[:, :128]
    plane_tot[1] = sums[:, 128:]
    plane_tots = []
    for i, off in enumerate(PLANE):
        row, col = at_plane(off)
        plane_tots.append(
            send(plane_tot.at[(row // 2) % 2], plane_tot.at[2 + i], tot_send.at[4 + i], tot_recv.at[4 + i], (row, col))
        )
    start_wave(3)
    whole = plane_tot[y_lo]
    for i in range(15):
        plane_tots[i].wait_recv()
        whole += plane_tot[2 + i]
    whole = jnp.sum(whole, axis=0, keepdims=True) * (1.0 / total_ents)
    share[...] = pltpu.roll(jnp.broadcast_to(whole, (8, 128)), (128 - d * 16) % 128, 1)

    for copy in slab_copies:
        copy.wait_recv()
    for copy in own_copies:
        copy.wait()
    sent = copies + list(x_copies.values()) + plane_copies + gath_copies + list(xg_copies.values())
    for copy in sent + pg_copies + [half] + list(x_tots.values()) + plane_tots + slab_copies:
        copy.wait_send()


def shards(entity_table, relations, thresholds, head_ids, rel_ids, thr_idx):
    ents, width = entity_table.shape
    n_rows, n_dim = lax.axis_size("rows"), lax.axis_size("dim")
    total_ents = ents * n_rows * n_dim
    slab = width // n_dim
    group = 256
    hbm = pl.BlockSpec(memory_space=pl.ANY)
    smem = pl.BlockSpec(memory_space=pltpu.SMEM)
    vmem = pl.BlockSpec(memory_space=pltpu.VMEM)
    dma = pltpu.SemaphoreType.DMA
    waves = len(WAVES)
    serving, share = pl.pallas_call(
        functools.partial(kernel, total_ents),
        out_shape=(
            jax.ShapeDtypeStruct((slab, ents * n_dim), F32),
            jax.ShapeDtypeStruct((8, 128), F32),
        ),
        in_specs=[smem, smem, smem, hbm, hbm, vmem],
        out_specs=(hbm, vmem),
        scratch_shapes=[
            pltpu.VMEM((ents, width), F32),
            pltpu.VMEM((width, ents), F32),
            pltpu.VMEM((ents, width), jnp.bfloat16),
            pltpu.VMEM(relations.shape, F32),
            pltpu.VMEM((4, group, width), F32),
            pltpu.VMEM((4, group, width), F32),
            pltpu.VMEM((4, group, width), F32),
            pltpu.VMEM((3, group, width), F32),
            pltpu.VMEM((15, 16, width), F32),
            pltpu.VMEM((16, width), F32),
            pltpu.VMEM((16, width), F32),
            pltpu.VMEM((8, group, width), F32),
            pltpu.VMEM((16, 128), F32),
            pltpu.VMEM((8, 8, group), F32),
            pltpu.VMEM((4, 8, group), F32),
            pltpu.VMEM((7, 8, group), F32),
            pltpu.VMEM((17, 8, 128), F32),
            dma((5,)),
            dma((waves,)),
            dma((waves, 7)), dma((waves, 7)),
            dma((4,)), dma((4,)),
            dma((3,)), dma((3,)),
            dma((15,)), dma((15,)),
            dma((15,)), dma((15,)),
            dma((3,)), dma((3,)),
            dma((4,)), dma((4,)),
            dma((19,)), dma((19,)),
        ],
        compiler_params=pltpu.CompilerParams(
            collective_id=0, has_side_effects=True, vmem_limit_bytes=60 * 1024 * 1024
        ),
        name="serve_and_count",
    )(head_ids, rel_ids, thresholds, entity_table, relations, thr_idx.reshape(16, 128))
    return serving.T, share[0, :16]


def solution(mesh):
    placed = (P(("rows", "dim"), None), P(), P(), P(), P(), P())
    return jax.shard_map(
        shards,
        mesh=mesh,
        in_specs=placed,
        out_specs=(P("rows", "dim"), P(("rows", "dim"))),
        check_vma=False,
    )
```

```python
import functools

import jax
import jax.numpy as jnp
from jax import lax
from jax.experimental import pallas as pl
from jax.experimental.pallas import tpu as pltpu
from jax.sharding import PartitionSpec as P

MESH = pl.DeviceIdType.MESH
F32 = jnp.float32
sharpness = 2.0

PLANE = [(a, b, z) for a in range(2) for b in range(2) for z in range(4)][1:]
SLABS = [(0, 0, 1), (0, 0, 3), (0, 1, 0), (0, 0, 2), (0, 1, 1), (0, 1, 3), (0, 1, 2)]
WAVES = [(0, 1152), (1152, 256), (1408, 1920), (3328, 768)]


def kernel(
    total_ents, head_ids, rel_ids, thresholds, table, relations, thr_idx,
    serving, share,
    tab, tab_t, ent, rel, theirs, mine, pair_in, x_in, plane_in, rel_rows, query_rows, queries,
    level, totals, pair_tot, x_tot, plane_tot,
    load_sem, slab_send, slab_recv, pair_send, pair_recv, x_send, x_recv,
    plane_send, plane_recv, gath_send, gath_recv, xg_send, xg_recv, pg_send, pg_recv,
    tot_send, tot_recv,
):
    r, d = lax.axis_index("rows"), lax.axis_index("dim")
    x, y_lo, core = r // 4, (r // 2) % 2, r % 2
    y_hi, z = d // 4, d % 4
    ents = table.shape[0]
    width = table.shape[1]
    group = x_in.shape[1]
    slab = serving.shape[0]

    def at_plane(off):
        a, b, dz = off
        row = x * 4 + ((y_lo + a) % 2) * 2 + core
        return row, ((y_hi + b) % 2) * 4 + (z + dz) % 4

    def at_x(k):
        return ((x + k) % 4) * 4 + y_lo * 2 + core, d

    partner = (x * 4 + y_lo * 2 + (1 - core), d)

    def send(src, dst, s, t, peer):
        copy = pltpu.make_async_remote_copy(
            src_ref=src, dst_ref=dst, send_sem=s, recv_sem=t, device_id=peer, device_id_type=MESH
        )
        copy.start()
        return copy

    cuts = [0, WAVES[0][1], 2048, 3072, ents]
    loads = []
    for k in range(4):
        span = pl.ds(cuts[k], cuts[k + 1] - cuts[k])
        loads.append(pltpu.make_async_copy(table.at[span], tab.at[span], load_sem.at[k]))
        loads[-1].start()
    load_rel = pltpu.make_async_copy(relations, rel, load_sem.at[4])
    load_rel.start()
    barrier = pltpu.get_barrier_semaphore()
    peers = [at_plane(off) for off in PLANE] + [at_x(k) for k in (1, 2, 3)] + [partner]
    for peer in peers:
        pl.semaphore_signal(barrier, inc=1, device_id=peer, device_id_type=MESH)

    def transpose_rows(first, count):
        @pl.loop(0, count // 128)
        def _(i):
            span = pl.ds(pl.multiple_of(first + i * 128, 128), 128)
            tab_t[:, span] = tab[span, :].T

    slab_copies = []

    def start_wave(w):
        first, count = WAVES[w]
        span = pl.ds(first, count)
        here = pl.ds(pl.multiple_of(d * ents + first, 128), count)
        for i, off in enumerate(SLABS):
            row, col = at_plane(off)
            rows = pl.ds(pl.multiple_of(col * slab, 8), slab)
            slab_copies.append(
                send(tab_t.at[rows, span], serving.at[:, here], slab_send.at[w, i], slab_recv.at[w, i], (row, col))
            )
        rows = pl.ds(pl.multiple_of(d * slab, 8), slab)
        serving[:, here] = tab_t[rows, span]

    loads[0].wait()
    transpose_rows(*WAVES[0])
    pl.semaphore_wait(barrier, len(peers))
    start_wave(0)
    for k in range(1, 4):
        loads[k].wait()

    start = (r * lax.axis_size("dim") + d) * ents
    tab[pl.ds(ents, 8), :] = jnp.zeros((8, width), F32)

    def pick(out, half, k):
        @pl.loop(0, group // 8)
        def _(i):
            rows = []
            for j in range(8):
                low = i * 8 + j
                q = k * 512 + (low // 128) * 256 + half * 128 + low % 128
                local = head_ids[q] - start
                missing = jnp.logical_or(local < 0, local >= ents)
                rows.append(tab[pl.ds(jnp.where(missing, ents, local), 1), :])
            out[k, pl.ds(pl.multiple_of(i * 8, 8), 8), :] = jnp.concatenate(rows, axis=0)

    order = [(x + 2) % 4, (x + 1) % 4, (x + 3) % 4, x]
    copies, x_copies = [], {}

    def sum_pair(n, k):
        copies[n].wait_recv()
        mine[order[n]] += pair_in[order[n]]
        if k:
            x_copies[k] = send(mine.at[order[n]], x_in.at[k - 1], x_send.at[k - 1], x_recv.at[k - 1], at_x(k))

    for n, k in enumerate((2, 1, 3, 0)):
        pick(theirs, 1 - core, order[n])
        copies.append(send(theirs.at[order[n]], pair_in.at[order[n]], pair_send.at[n], pair_recv.at[n], partner))
        if n:
            sum_pair(n - 1, (2, 1, 3, 0)[n - 1])
        pick(mine, core, order[n])
    sum_pair(3, 0)

    transpose_rows(WAVES[0][1], ents - WAVES[0][1])

    @pl.loop(0, ents // 256)
    def _(i):
        span = pl.ds(pl.multiple_of(i * 256, 256), 256)
        ent[span, :] = tab[span, :].astype(jnp.bfloat16)

    found = jnp.zeros(level.shape, F32)
    for k in range(thresholds.shape[0]):
        found = jnp.where(thr_idx[...] == k, thresholds[k], found)
    level[...] = found
    load_rel.wait()
    first_q = r * 128 + d * 16
    for i in range(16):
        rel_rows[pl.ds(i, 1), :] = rel[pl.ds(rel_ids[first_q + i], 1), :]

    for k in (1, 3, 2):
        x_copies[k].wait_recv()
        mine[x] += x_in[k - 1]

    def rows_of(row, col):
        return pl.ds(pl.multiple_of(((row // 2) % 2) * 128 + col * 16, 16), 16)

    plane_copies = []
    for i, off in enumerate(PLANE):
        peer = at_plane(off)
        plane_copies.append(
            send(mine.at[x, rows_of(*peer)], plane_in.at[i], plane_send.at[i], plane_recv.at[i], peer)
        )
    start_wave(1)
    head = mine[x, rows_of(r, d)]
    for i in range(15):
        plane_copies[i].wait_recv()
        head += plane_in[i]

    query_rows[...] = (head * rel_rows[...]).astype(jnp.bfloat16).astype(F32)
    own_group = core * 4 + x
    gath_copies = []
    for i, off in enumerate(PLANE):
        gath_copies.append(
            send(query_rows, queries.at[own_group, rows_of(r, d)], gath_send.at[i], gath_recv.at[i], at_plane(off))
        )
    start_wave(2)
    queries[own_group, rows_of(r, d)] = query_rows[...]
    for i in range(15):
        gath_copies[i].wait_recv()

    xg_copies = {}
    for k in (1, 3, 2):
        xg_copies[k] = send(queries.at[own_group], queries.at[own_group], xg_send.at[k - 1], xg_recv.at[k - 1], at_x(k))

    tile = 512

    def count(half, k):
        g = half * 4 + k
        low = queries[g].astype(jnp.bfloat16)
        lev = jnp.concatenate(
            [level[pl.ds(k * 4 + half, 1), :], level[pl.ds(k * 4 + 2 + half, 1), :]], axis=1
        )

        def step(i, acc):
            rows = ent[pl.ds(pl.multiple_of(i * tile, tile), tile), :]
            score = lax.dot_general(rows, low, (((1,), (1,)), ((), ())), preferred_element_type=F32)
            soft = 1.0 / (1.0 + jnp.exp(sharpness * (lev - score)))
            return acc + jnp.sum(soft.reshape(tile // 8, 8, group), axis=0)

        totals[g] = lax.fori_loop(0, ents // tile, step, jnp.zeros((8, group), F32))

    pg_copies = []
    for n, k in enumerate((0, 1, 3, 2)):
        from_x = (x + 4 - k) % 4
        if k:
            xg_copies[k].wait_recv()
        g = core * 4 + from_x
        pg_copies.append(send(queries.at[g], queries.at[g], pg_send.at[n], pg_recv.at[n], partner))
        count(core, from_x)
        pg_copies[n].wait_recv()
        count(1 - core, from_x)

    other = pl.ds((1 - core) * 4, 4)
    half = send(totals.at[other], pair_tot, tot_send.at[0], tot_recv.at[0], partner)
    half.wait_recv()
    x_tots = {}
    for k in (0, 1, 2, 3):
        to = (x + k) % 4
        x_tot[k] = totals[core * 4 + to] + pair_tot[to]
        if k:
            x_tots[k] = send(x_tot.at[k], x_tot.at[3 + k], tot_send.at[k], tot_recv.at[k], at_x(k))
    sums = x_tot[0]
    for k in (1, 2, 3):
        x_tots[k].wait_recv()
        sums += x_tot[3 + k]
    plane_tot[0] = sums[:, :128]
    plane_tot[1] = sums[:, 128:]
    plane_tots = []
    for i, off in enumerate(PLANE):
        row, col = at_plane(off)
        plane_tots.append(
            send(plane_tot.at[(row // 2) % 2], plane_tot.at[2 + i], tot_send.at[4 + i], tot_recv.at[4 + i], (row, col))
        )
    start_wave(3)
    whole = plane_tot[y_lo]
    for i in range(15):
        plane_tots[i].wait_recv()
        whole += plane_tot[2 + i]
    whole = jnp.sum(whole, axis=0, keepdims=True) * (1.0 / total_ents)
    share[...] = pltpu.roll(jnp.broadcast_to(whole, (8, 128)), (128 - d * 16) % 128, 1)

    for copy in slab_copies:
        copy.wait_recv()
    sent = copies + list(x_copies.values()) + plane_copies + gath_copies + list(xg_copies.values())
    for copy in sent + pg_copies + [half] + list(x_tots.values()) + plane_tots + slab_copies:
        copy.wait_send()


def write_out(landed, share, serving, fraction, sems):
    copies = []
    for i in range(8):
        rows = pl.ds(i * (landed.shape[0] // 8), landed.shape[0] // 8)
        copies.append(pltpu.make_async_copy(landed.at[rows], serving.at[rows], sems.at[i]))
        copies[-1].start()
    fraction[...] = share[0, :16]
    for copy in copies:
        copy.wait()


def shards(entity_table, relations, thresholds, head_ids, rel_ids, thr_idx):
    ents, width = entity_table.shape
    n_rows, n_dim = lax.axis_size("rows"), lax.axis_size("dim")
    total_ents = ents * n_rows * n_dim
    slab = width // n_dim
    group = 256
    hbm = pl.BlockSpec(memory_space=pl.ANY)
    smem = pl.BlockSpec(memory_space=pltpu.SMEM)
    vmem = pl.BlockSpec(memory_space=pltpu.VMEM)
    dma = pltpu.SemaphoreType.DMA
    waves = len(WAVES)
    landed, share = pl.pallas_call(
        functools.partial(kernel, total_ents),
        out_shape=(
            pltpu.VMEM((slab, ents * n_dim), F32),
            pltpu.VMEM((8, 128), F32),
        ),
        in_specs=[smem, smem, smem, hbm, hbm, vmem],
        out_specs=(vmem, vmem),
        scratch_shapes=[
            pltpu.VMEM((ents + 8, width), F32),
            pltpu.VMEM((width, ents), F32),
            pltpu.VMEM((ents, width), jnp.bfloat16),
            pltpu.VMEM(relations.shape, F32),
            pltpu.VMEM((4, group, width), F32),
            pltpu.VMEM((4, group, width), F32),
            pltpu.VMEM((4, group, width), F32),
            pltpu.VMEM((3, group, width), F32),
            pltpu.VMEM((15, 16, width), F32),
            pltpu.VMEM((16, width), F32),
            pltpu.VMEM((16, width), F32),
            pltpu.VMEM((8, group, width), F32),
            pltpu.VMEM((16, 128), F32),
            pltpu.VMEM((8, 8, group), F32),
            pltpu.VMEM((4, 8, group), F32),
            pltpu.VMEM((7, 8, group), F32),
            pltpu.VMEM((17, 8, 128), F32),
            dma((5,)),
            dma((waves, 7)), dma((waves, 7)),
            dma((4,)), dma((4,)),
            dma((3,)), dma((3,)),
            dma((15,)), dma((15,)),
            dma((15,)), dma((15,)),
            dma((3,)), dma((3,)),
            dma((4,)), dma((4,)),
            dma((19,)), dma((19,)),
        ],
        compiler_params=pltpu.CompilerParams(
            collective_id=0, has_side_effects=True, vmem_limit_bytes=48 * 1024 * 1024
        ),
        name="serve_and_count",
    )(head_ids, rel_ids, thresholds, entity_table, relations, thr_idx.reshape(16, 128))
    serving, fraction = pl.pallas_call(
        write_out,
        out_shape=(
            jax.ShapeDtypeStruct((slab, ents * n_dim), F32),
            jax.ShapeDtypeStruct((16,), F32),
        ),
        in_specs=[vmem, vmem],
        out_specs=(hbm, vmem),
        scratch_shapes=[dma((8,))],
        compiler_params=pltpu.CompilerParams(vmem_limit_bytes=1024 * 1024),
        name="write_out",
    )(landed, share)
    return serving.T, fraction


def solution(mesh):
    placed = (P(("rows", "dim"), None), P(), P(), P(), P(), P())
    return jax.shard_map(
        shards,
        mesh=mesh,
        in_specs=placed,
        out_specs=(P("rows", "dim"), P(("rows", "dim"))),
        check_vma=False,
    )
```

```python
import functools

import jax
import jax.numpy as jnp
from jax import lax
from jax.experimental import pallas as pl
from jax.experimental.pallas import tpu as pltpu
from jax.sharding import PartitionSpec as P

MESH = pl.DeviceIdType.MESH
F32 = jnp.float32
sharpness = 2.0

PLANE = [(a, b, z) for a in range(2) for b in range(2) for z in range(4)][1:]
SLABS = [(0, 1, 2), (0, 0, 2), (0, 1, 1), (0, 1, 3), (0, 1, 0), (0, 0, 1), (0, 0, 3)]
COUNTS = [1152, 256, 256, 768, 128, 256, 128, 128, 256, 128, 128, 256, 256]
WAVES = [(sum(COUNTS[:k]), COUNTS[k]) for k in range(len(COUNTS))]


def kernel(
    total_ents, head_ids_in, rel_ids_in, thresholds_in, table, relations, thr_idx_in,
    serving, share,
    head_ids, rel_ids, thresholds, thr_idx,
    tab, tab_t, ent, rel, theirs, mine, pair_in, x_in, plane_in, rel_rows, query_rows, queries,
    level, totals, pair_tot, x_tot, plane_tot,
    load_sem, slab_send, slab_recv, pair_send, pair_recv, x_send, x_recv,
    plane_send, plane_recv, gath_send, gath_recv, xg_send, xg_recv, pg_send, pg_recv,
    tot_send, tot_recv,
):
    r, d = lax.axis_index("rows"), lax.axis_index("dim")
    x, y_lo, core = r // 4, (r // 2) % 2, r % 2
    y_hi, z = d // 4, d % 4
    ents = table.shape[0]
    width = table.shape[1]
    group = x_in.shape[1]
    slab = serving.shape[0]

    def at_plane(off):
        a, b, dz = off
        row = x * 4 + ((y_lo + a) % 2) * 2 + core
        return row, ((y_hi + b) % 2) * 4 + (z + dz) % 4

    def at_x(k):
        return ((x + k) % 4) * 4 + y_lo * 2 + core, d

    partner = (x * 4 + y_lo * 2 + (1 - core), d)

    def send(src, dst, s, t, peer):
        copy = pltpu.make_async_remote_copy(
            src_ref=src, dst_ref=dst, send_sem=s, recv_sem=t, device_id=peer, device_id_type=MESH
        )
        copy.start()
        return copy

    cuts = [0, COUNTS[0], 2048, 3072, ents]
    loads = []
    for k in range(4):
        span = pl.ds(cuts[k], cuts[k + 1] - cuts[k])
        loads.append(pltpu.make_async_copy(table.at[span], tab.at[span], load_sem.at[k]))
        loads[-1].start()
    small = []
    for i, (src, dst) in enumerate(
        ((head_ids_in, head_ids), (rel_ids_in, rel_ids), (thresholds_in, thresholds), (thr_idx_in, thr_idx), (relations, rel))
    ):
        small.append(pltpu.make_async_copy(src, dst, load_sem.at[4 + i]))
        small[-1].start()
    barrier = pltpu.get_barrier_semaphore()
    peers = [at_plane(off) for off in PLANE] + [at_x(k) for k in (1, 2, 3)] + [partner]
    for peer in peers:
        pl.semaphore_signal(barrier, inc=1, device_id=peer, device_id_type=MESH)

    def transpose_rows(first, count):
        @pl.loop(0, count // 128)
        def _(i):
            span = pl.ds(pl.multiple_of(first + i * 128, 128), 128)
            tab_t[:, span] = tab[span, :].T

    slab_copies = []

    def start_wave(w):
        first, count = WAVES[w]
        span = pl.ds(first, count)
        here = pl.ds(pl.multiple_of(d * ents + first, 128), count)
        for i, off in enumerate(SLABS):
            row, col = at_plane(off)
            rows = pl.ds(pl.multiple_of(col * slab, 8), slab)
            slab_copies.append(
                send(tab_t.at[rows, span], serving.at[:, here], slab_send.at[w, i], slab_recv.at[w, i], (row, col))
            )
        rows = pl.ds(pl.multiple_of(d * slab, 8), slab)
        serving[:, here] = tab_t[rows, span]

    loads[0].wait()
    transpose_rows(*WAVES[0])
    pl.semaphore_wait(barrier, len(peers))
    start_wave(0)
    for k in range(1, 4):
        loads[k].wait()
    small[0].wait()

    start = (r * lax.axis_size("dim") + d) * ents
    tab[pl.ds(ents, 8), :] = jnp.zeros((8, width), F32)

    def pick(out, half, k):
        for part in range(2):
            base = k * 512 + part * 256 + half * 128

            @pl.loop(0, 16)
            def _(i):
                rows = []
                for j in range(8):
                    local = (head_ids[base + i * 8 + j] - start).astype(jnp.uint32)
                    row = jnp.minimum(local, jnp.uint32(ents)).astype(jnp.int32)
                    rows.append(tab[pl.ds(row, 1), :])
                span = pl.ds(pl.multiple_of(part * 128 + i * 8, 8), 8)
                out[k, span, :] = jnp.concatenate(rows, axis=0)

    order = [(x + 2) % 4, (x + 1) % 4, (x + 3) % 4, x]
    copies, x_copies = [], {}

    def sum_pair(n, k):
        copies[n].wait_recv()
        mine[order[n]] += pair_in[order[n]]
        if k:
            x_copies[k] = send(mine.at[order[n]], x_in.at[k - 1], x_send.at[k - 1], x_recv.at[k - 1], at_x(k))

    for n, k in enumerate((2, 1, 3, 0)):
        pick(theirs, 1 - core, order[n])
        copies.append(send(theirs.at[order[n]], pair_in.at[order[n]], pair_send.at[n], pair_recv.at[n], partner))
        if n:
            sum_pair(n - 1, (2, 1, 3, 0)[n - 1])
        pick(mine, core, order[n])
    sum_pair(3, 0)

    transpose_rows(WAVES[0][1], ents - WAVES[0][1])

    @pl.loop(0, ents // 256)
    def _(i):
        span = pl.ds(pl.multiple_of(i * 256, 256), 256)
        ent[span, :] = tab[span, :].astype(jnp.bfloat16)

    for copy in small[1:]:
        copy.wait()
    found = jnp.zeros(level.shape, F32)
    for k in range(thresholds.shape[0]):
        found = jnp.where(thr_idx[...] == k, thresholds[k], found)
    level[...] = found
    first_q = r * 128 + d * 16
    for i in range(16):
        rel_rows[pl.ds(i, 1), :] = rel[pl.ds(rel_ids[first_q + i], 1), :]

    for k in (1, 3, 2):
        x_copies[k].wait_recv()
        mine[x] += x_in[k - 1]

    def rows_of(row, col):
        return pl.ds(pl.multiple_of(((row // 2) % 2) * 128 + col * 16, 16), 16)

    plane_copies = []
    for i, off in enumerate(PLANE):
        peer = at_plane(off)
        plane_copies.append(
            send(mine.at[x, rows_of(*peer)], plane_in.at[i], plane_send.at[i], plane_recv.at[i], peer)
        )
    start_wave(1)
    head = mine[x, rows_of(r, d)]
    for i in range(15):
        plane_copies[i].wait_recv()
        head += plane_in[i]

    query_rows[...] = (head * rel_rows[...]).astype(jnp.bfloat16).astype(F32)
    own_group = core * 4 + x
    gath_copies = []
    for i, off in enumerate(PLANE):
        gath_copies.append(
            send(query_rows, queries.at[own_group, rows_of(r, d)], gath_send.at[i], gath_recv.at[i], at_plane(off))
        )
    start_wave(2)
    queries[own_group, rows_of(r, d)] = query_rows[...]
    for i in range(15):
        gath_copies[i].wait_recv()

    xg_copies = {}

    def gather_x(k):
        xg_copies[k] = send(
            queries.at[own_group], queries.at[own_group], xg_send.at[k - 1], xg_recv.at[k - 1], at_x(k)
        )

    gather_x(1)
    gather_x(3)
    start_wave(3)
    tile = 512

    def count(half, k):
        g = half * 4 + k
        low = queries[g].astype(jnp.bfloat16)
        lev = jnp.concatenate(
            [level[pl.ds(k * 4 + half, 1), :], level[pl.ds(k * 4 + 2 + half, 1), :]], axis=1
        )

        def step(i, acc):
            rows = ent[pl.ds(pl.multiple_of(i * tile, tile), tile), :]
            score = lax.dot_general(rows, low, (((1,), (1,)), ((), ())), preferred_element_type=F32)
            soft = 1.0 / (1.0 + jnp.exp(sharpness * (lev - score)))
            return acc + jnp.sum(soft.reshape(tile // 8, 8, group), axis=0)

        totals[g] = lax.fori_loop(0, ents // tile, step, jnp.zeros((8, group), F32))

    pg_copies = []

    def pass_on(n, k):
        g = core * 4 + (x + 4 - k) % 4
        pg_copies.append(send(queries.at[g], queries.at[g], pg_send.at[n], pg_recv.at[n], partner))

    def both(n, k):
        from_x = (x + 4 - k) % 4
        count(core, from_x)
        start_wave(4 + 2 * n)
        pg_copies[n].wait_recv()
        count(1 - core, from_x)
        start_wave(5 + 2 * n)

    pass_on(0, 0)
    both(0, 0)
    xg_copies[1].wait_recv()
    xg_copies[3].wait_recv()
    gather_x(2)
    pass_on(1, 1)
    pass_on(2, 3)
    both(1, 1)
    both(2, 3)
    xg_copies[2].wait_recv()
    pass_on(3, 2)
    both(3, 2)

    other = pl.ds((1 - core) * 4, 4)
    half = send(totals.at[other], pair_tot, tot_send.at[0], tot_recv.at[0], partner)
    half.wait_recv()
    x_tots = {}
    for k in (0, 1, 2, 3):
        to = (x + k) % 4
        x_tot[k] = totals[core * 4 + to] + pair_tot[to]
        if k:
            x_tots[k] = send(x_tot.at[k], x_tot.at[3 + k], tot_send.at[k], tot_recv.at[k], at_x(k))
    sums = x_tot[0]
    for k in (1, 2, 3):
        x_tots[k].wait_recv()
        sums += x_tot[3 + k]
    plane_tot[0] = sums[:, :128]
    plane_tot[1] = sums[:, 128:]
    plane_tots = []
    for i, off in enumerate(PLANE):
        row, col = at_plane(off)
        plane_tots.append(
            send(plane_tot.at[(row // 2) % 2], plane_tot.at[2 + i], tot_send.at[4 + i], tot_recv.at[4 + i], (row, col))
        )
    start_wave(12)
    whole = plane_tot[y_lo]
    for i in range(15):
        plane_tots[i].wait_recv()
        whole += plane_tot[2 + i]
    whole = jnp.sum(whole, axis=0, keepdims=True) * (1.0 / total_ents)
    share[...] = pltpu.roll(jnp.broadcast_to(whole, (8, 128)), (128 - d * 16) % 128, 1)

    for copy in slab_copies:
        copy.wait_recv()
    sent = copies + list(x_copies.values()) + plane_copies + gath_copies + list(xg_copies.values())
    for copy in sent + pg_copies + [half] + list(x_tots.values()) + plane_tots + slab_copies:
        copy.wait_send()


def write_out(landed, share, serving, fraction, sems):
    copies = []
    for i in range(8):
        rows = pl.ds(i * (landed.shape[0] // 8), landed.shape[0] // 8)
        copies.append(pltpu.make_async_copy(landed.at[rows], serving.at[rows], sems.at[i]))
        copies[-1].start()
    fraction[...] = share[0, :16]
    for copy in copies:
        copy.wait()


def shards(entity_table, relations, thresholds, head_ids, rel_ids, thr_idx):
    ents, width = entity_table.shape
    n_rows, n_dim = lax.axis_size("rows"), lax.axis_size("dim")
    total_ents = ents * n_rows * n_dim
    slab = width // n_dim
    group = 256
    hbm = pl.BlockSpec(memory_space=pl.ANY)
    vmem = pl.BlockSpec(memory_space=pltpu.VMEM)
    dma = pltpu.SemaphoreType.DMA
    waves = len(WAVES)
    landed, share = pl.pallas_call(
        functools.partial(kernel, total_ents),
        out_shape=(
            pltpu.VMEM((slab, ents * n_dim), F32),
            pltpu.VMEM((8, 128), F32),
        ),
        in_specs=[hbm] * 6,
        out_specs=(vmem, vmem),
        scratch_shapes=[
            pltpu.SMEM(head_ids.shape, jnp.int32),
            pltpu.SMEM(rel_ids.shape, jnp.int32),
            pltpu.SMEM(thresholds.shape, F32),
            pltpu.VMEM((16, 128), jnp.int32),
            pltpu.VMEM((ents + 8, width), F32),
            pltpu.VMEM((width, ents), F32),
            pltpu.VMEM((ents, width), jnp.bfloat16),
            pltpu.VMEM(relations.shape, F32),
            pltpu.VMEM((4, group, width), F32),
            pltpu.VMEM((4, group, width), F32),
            pltpu.VMEM((4, group, width), F32),
            pltpu.VMEM((3, group, width), F32),
            pltpu.VMEM((15, 16, width), F32),
            pltpu.VMEM((16, width), F32),
            pltpu.VMEM((16, width), F32),
            pltpu.VMEM((8, group, width), F32),
            pltpu.VMEM((16, 128), F32),
            pltpu.VMEM((8, 8, group), F32),
            pltpu.VMEM((4, 8, group), F32),
            pltpu.VMEM((7, 8, group), F32),
            pltpu.VMEM((17, 8, 128), F32),
            dma((9,)),
            dma((waves, 7)), dma((waves, 7)),
            dma((4,)), dma((4,)),
            dma((3,)), dma((3,)),
            dma((15,)), dma((15,)),
            dma((15,)), dma((15,)),
            dma((3,)), dma((3,)),
            dma((4,)), dma((4,)),
            dma((19,)), dma((19,)),
        ],
        compiler_params=pltpu.CompilerParams(
            collective_id=0, has_side_effects=True, vmem_limit_bytes=48 * 1024 * 1024
        ),
        name="serve_and_count",
    )(head_ids, rel_ids, thresholds, entity_table, relations, thr_idx.reshape(16, 128))
    serving, fraction = pl.pallas_call(
        write_out,
        out_shape=(
            jax.ShapeDtypeStruct((slab, ents * n_dim), F32),
            jax.ShapeDtypeStruct((16,), F32),
        ),
        in_specs=[vmem, vmem],
        out_specs=(hbm, vmem),
        scratch_shapes=[dma((8,))],
        compiler_params=pltpu.CompilerParams(vmem_limit_bytes=1024 * 1024),
        name="write_out",
    )(landed, share)
    return serving.T, fraction


def solution(mesh):
    placed = (P(("rows", "dim"), None), P(), P(), P(), P(), P())
    return jax.shard_map(
        shards,
        mesh=mesh,
        in_specs=placed,
        out_specs=(P("rows", "dim"), P(("rows", "dim"))),
        check_vma=False,
    )
```

```python
import functools

import jax
import jax.numpy as jnp
from jax import lax
from jax.experimental import pallas as pl
from jax.experimental.pallas import tpu as pltpu
from jax.sharding import PartitionSpec as P

MESH = pl.DeviceIdType.MESH
F32 = jnp.float32
sharpness = 2.0

PLANE = [(a, b, z) for a in range(2) for b in range(2) for z in range(4)][1:]
SLABS = [(0, 1, 2), (0, 0, 2), (0, 1, 1), (0, 1, 3), (0, 1, 0), (0, 0, 1), (0, 0, 3)]
COUNTS = [1152, 256, 256, 768, 128, 256, 128, 128, 256, 128, 128, 256, 256]
WAVES = [(sum(COUNTS[:k]), COUNTS[k]) for k in range(len(COUNTS))]


def kernel(
    total_ents, head_ids_in, rel_ids_in, thresholds_in, table, relations, thr_idx_in,
    serving, share,
    head_ids, rel_ids, thresholds, thr_idx,
    tab, tab_t, ent, rel, theirs, mine, pair_in, x_in, plane_in, rel_rows, query_rows, queries,
    level, totals, pair_tot, x_tot, plane_tot,
    load_sem, slab_send, slab_recv, pair_send, pair_recv, x_send, x_recv,
    plane_send, plane_recv, gath_send, gath_recv, xg_send, xg_recv, pg_send, pg_recv,
    tot_send, tot_recv, last_send, last_recv,
):
    r, d = lax.axis_index("rows"), lax.axis_index("dim")
    x, y_lo, core = r // 4, (r // 2) % 2, r % 2
    y_hi, z = d // 4, d % 4
    ents = table.shape[0]
    width = table.shape[1]
    group = x_in.shape[1]
    slab = serving.shape[0]

    def at_plane(off):
        a, b, dz = off
        row = x * 4 + ((y_lo + a) % 2) * 2 + core
        return row, ((y_hi + b) % 2) * 4 + (z + dz) % 4

    def at_x(k):
        return ((x + k) % 4) * 4 + y_lo * 2 + core, d

    partner = (x * 4 + y_lo * 2 + (1 - core), d)

    def send(src, dst, s, t, peer):
        copy = pltpu.make_async_remote_copy(
            src_ref=src, dst_ref=dst, send_sem=s, recv_sem=t, device_id=peer, device_id_type=MESH
        )
        copy.start()
        return copy

    def all_of(src, dst, s, t):
        return pltpu.make_async_remote_copy(
            src_ref=src, dst_ref=dst, send_sem=s, recv_sem=t, device_id=partner, device_id_type=MESH
        )

    cuts = [0, COUNTS[0], 2048, 3072, ents]
    loads = []
    for k in range(4):
        span = pl.ds(cuts[k], cuts[k + 1] - cuts[k])
        loads.append(pltpu.make_async_copy(table.at[span], tab.at[span], load_sem.at[k]))
        loads[-1].start()
    small = []
    for i, (src, dst) in enumerate(
        ((head_ids_in, head_ids), (rel_ids_in, rel_ids), (thresholds_in, thresholds), (thr_idx_in, thr_idx), (relations, rel))
    ):
        small.append(pltpu.make_async_copy(src, dst, load_sem.at[4 + i]))
        small[-1].start()
    barrier = pltpu.get_barrier_semaphore()
    peers = [at_plane(off) for off in PLANE] + [at_x(k) for k in (1, 2, 3)] + [partner]
    for peer in peers:
        pl.semaphore_signal(barrier, inc=1, device_id=peer, device_id_type=MESH)

    def transpose_rows(first, count):
        @pl.loop(0, count // 128)
        def _(i):
            span = pl.ds(pl.multiple_of(first + i * 128, 128), 128)
            tab_t[:, span] = tab[span, :].T

    def start_wave(w):
        first, count = WAVES[w]
        span = pl.ds(first, count)
        here = pl.ds(pl.multiple_of(d * ents + first, 128), count)
        for off in SLABS:
            row, col = at_plane(off)
            rows = pl.ds(pl.multiple_of(col * slab, 8), slab)
            send(tab_t.at[rows, span], serving.at[:, here], slab_send, slab_recv, (row, col))
        rows = pl.ds(pl.multiple_of(d * slab, 8), slab)
        serving[:, here] = tab_t[rows, span]

    loads[0].wait()
    transpose_rows(*WAVES[0])
    pl.semaphore_wait(barrier, len(peers))
    start_wave(0)
    for k in range(1, 4):
        loads[k].wait()
    small[0].wait()

    start = (r * lax.axis_size("dim") + d) * ents
    tab[pl.ds(ents, 8), :] = jnp.zeros((8, width), F32)

    def pick(out, half, k):
        for part in range(2):
            base = k * 512 + part * 256 + half * 128

            @pl.loop(0, 16)
            def _(i):
                rows = []
                for j in range(8):
                    local = (head_ids[base + i * 8 + j] - start).astype(jnp.uint32)
                    row = jnp.minimum(local, jnp.uint32(ents)).astype(jnp.int32)
                    rows.append(tab[pl.ds(row, 1), :])
                span = pl.ds(pl.multiple_of(part * 128 + i * 8, 8), 8)
                out[k, span, :] = jnp.concatenate(rows, axis=0)

    order = [(x + 2) % 4, (x + 1) % 4, (x + 3) % 4, x]
    copies, x_copies = [], {}

    def sum_pair(n, k):
        copies[n].wait_recv()
        mine[order[n]] += pair_in[order[n]]
        if k:
            x_copies[k] = send(mine.at[order[n]], x_in.at[k - 1], x_send.at[k - 1], x_recv.at[k - 1], at_x(k))

    for n, k in enumerate((2, 1, 3, 0)):
        pick(theirs, 1 - core, order[n])
        copies.append(send(theirs.at[order[n]], pair_in.at[order[n]], pair_send.at[n], pair_recv.at[n], partner))
        if n:
            sum_pair(n - 1, (2, 1, 3, 0)[n - 1])
        pick(mine, core, order[n])
    sum_pair(3, 0)

    transpose_rows(WAVES[0][1], ents - WAVES[0][1])

    @pl.loop(0, ents // 256)
    def _(i):
        span = pl.ds(pl.multiple_of(i * 256, 256), 256)
        ent[span, :] = tab[span, :].astype(jnp.bfloat16)

    for copy in small[1:]:
        copy.wait()
    found = jnp.zeros(level.shape, F32)
    for k in range(thresholds.shape[0]):
        found = jnp.where(thr_idx[...] == k, thresholds[k], found)
    level[...] = found
    first_q = r * 128 + d * 16
    for i in range(16):
        rel_rows[pl.ds(i, 1), :] = rel[pl.ds(rel_ids[first_q + i], 1), :]

    for k in (1, 3, 2):
        x_copies[k].wait_recv()
        mine[x] += x_in[k - 1]

    def rows_of(row, col):
        return pl.ds(pl.multiple_of(((row // 2) % 2) * 128 + col * 16, 16), 16)

    for i, off in enumerate(PLANE):
        peer = at_plane(off)
        send(mine.at[x, rows_of(*peer)], plane_in.at[i], plane_send, plane_recv, peer)
    start_wave(1)
    head = mine[x, rows_of(r, d)]
    all_of(mine.at[x, pl.ds(0, 240)], plane_in, plane_send, plane_recv).wait_recv()
    for i in range(15):
        head += plane_in[i]

    query_rows[...] = (head * rel_rows[...]).astype(jnp.bfloat16).astype(F32)
    own_group = core * 4 + x
    for off in PLANE:
        send(query_rows, queries.at[own_group, rows_of(r, d)], gath_send, gath_recv, at_plane(off))
    start_wave(2)
    queries[own_group, rows_of(r, d)] = query_rows[...]
    gathered = all_of(mine.at[x, pl.ds(0, 240)], queries.at[own_group, pl.ds(0, 240)], gath_send, gath_recv)
    gathered.wait_recv()

    xg_copies = {}

    def gather_x(k):
        xg_copies[k] = send(
            queries.at[own_group], queries.at[own_group], xg_send.at[k - 1], xg_recv.at[k - 1], at_x(k)
        )

    gather_x(1)
    gather_x(3)
    start_wave(3)
    tile = 512

    def count(half, k):
        g = half * 4 + k
        low = queries[g].astype(jnp.bfloat16)
        lev = jnp.concatenate(
            [level[pl.ds(k * 4 + half, 1), :], level[pl.ds(k * 4 + 2 + half, 1), :]], axis=1
        )

        def step(i, acc):
            rows = ent[pl.ds(pl.multiple_of(i * tile, tile), tile), :]
            score = lax.dot_general(rows, low, (((1,), (1,)), ((), ())), preferred_element_type=F32)
            soft = 1.0 / (1.0 + jnp.exp(sharpness * (lev - score)))
            return acc + jnp.sum(soft.reshape(tile // 8, 8, group), axis=0)

        totals[g] = lax.fori_loop(0, ents // tile, step, jnp.zeros((8, group), F32))

    pg_copies = []

    def pass_on(n, k):
        g = core * 4 + (x + 4 - k) % 4
        pg_copies.append(send(queries.at[g], queries.at[g], pg_send.at[n], pg_recv.at[n], partner))

    def both(n, k):
        from_x = (x + 4 - k) % 4
        count(core, from_x)
        start_wave(4 + 2 * n)
        pg_copies[n].wait_recv()
        count(1 - core, from_x)
        start_wave(5 + 2 * n)

    pass_on(0, 0)
    both(0, 0)
    xg_copies[1].wait_recv()
    xg_copies[3].wait_recv()
    gather_x(2)
    pass_on(1, 1)
    pass_on(2, 3)
    both(1, 1)
    both(2, 3)
    xg_copies[2].wait_recv()
    pass_on(3, 2)
    both(3, 2)

    for copy in copies + list(x_copies.values()) + list(xg_copies.values()) + pg_copies:
        copy.wait_send()
    all_of(mine.at[x, pl.ds(0, 240)], plane_in, plane_send, plane_recv).wait_send()
    gathered.wait_send()

    other = pl.ds((1 - core) * 4, 4)
    half = send(totals.at[other], pair_tot, tot_send.at[0], tot_recv.at[0], partner)
    half.wait_recv()
    x_tots = {}
    for k in (0, 1, 2, 3):
        to = (x + k) % 4
        x_tot[k] = totals[core * 4 + to] + pair_tot[to]
        if k:
            x_tots[k] = send(x_tot.at[k], x_tot.at[3 + k], tot_send.at[k], tot_recv.at[k], at_x(k))
    sums = x_tot[0]
    for k in (1, 2, 3):
        x_tots[k].wait_recv()
        sums += x_tot[3 + k]
    plane_tot[0] = sums[:, :128]
    plane_tot[1] = sums[:, 128:]
    for i, off in enumerate(PLANE):
        row, col = at_plane(off)
        send(plane_tot.at[(row // 2) % 2], plane_tot.at[2 + i], last_send, last_recv, (row, col))
    start_wave(12)
    whole = plane_tot[y_lo]
    last = all_of(plane_tot.at[pl.ds(0, 15)], plane_tot.at[pl.ds(2, 15)], last_send, last_recv)
    last.wait_recv()
    half.wait_send()
    for k in (1, 2, 3):
        x_tots[k].wait_send()
    for i in range(15):
        whole += plane_tot[2 + i]
    whole = jnp.sum(whole, axis=0, keepdims=True) * (1.0 / total_ents)
    share[...] = pltpu.roll(jnp.broadcast_to(whole, (8, 128)), (128 - d * 16) % 128, 1)

    slabs = all_of(tab_t.at[pl.ds(0, 7 * slab)], serving.at[:, pl.ds(0, 7 * ents)], slab_send, slab_recv)
    slabs.wait_recv()
    slabs.wait_send()
    last.wait_send()


def write_out(landed, share, serving, fraction, sems):
    copies = []
    for i in range(8):
        rows = pl.ds(i * (landed.shape[0] // 8), landed.shape[0] // 8)
        copies.append(pltpu.make_async_copy(landed.at[rows], serving.at[rows], sems.at[i]))
        copies[-1].start()
    fraction[...] = share[0, :16]
    for copy in copies:
        copy.wait()


def shards(entity_table, relations, thresholds, head_ids, rel_ids, thr_idx):
    ents, width = entity_table.shape
    n_rows, n_dim = lax.axis_size("rows"), lax.axis_size("dim")
    total_ents = ents * n_rows * n_dim
    slab = width // n_dim
    group = 256
    hbm = pl.BlockSpec(memory_space=pl.ANY)
    vmem = pl.BlockSpec(memory_space=pltpu.VMEM)
    dma = pltpu.SemaphoreType.DMA
    landed, share = pl.pallas_call(
        functools.partial(kernel, total_ents),
        out_shape=(
            pltpu.VMEM((slab, ents * n_dim), F32),
            pltpu.VMEM((8, 128), F32),
        ),
        in_specs=[hbm] * 6,
        out_specs=(vmem, vmem),
        scratch_shapes=[
            pltpu.SMEM(head_ids.shape, jnp.int32),
            pltpu.SMEM(rel_ids.shape, jnp.int32),
            pltpu.SMEM(thresholds.shape, F32),
            pltpu.VMEM((16, 128), jnp.int32),
            pltpu.VMEM((ents + 8, width), F32),
            pltpu.VMEM((width, ents), F32),
            pltpu.VMEM((ents, width), jnp.bfloat16),
            pltpu.VMEM(relations.shape, F32),
            pltpu.VMEM((4, group, width), F32),
            pltpu.VMEM((4, group, width), F32),
            pltpu.VMEM((4, group, width), F32),
            pltpu.VMEM((3, group, width), F32),
            pltpu.VMEM((15, 16, width), F32),
            pltpu.VMEM((16, width), F32),
            pltpu.VMEM((16, width), F32),
            pltpu.VMEM((8, group, width), F32),
            pltpu.VMEM((16, 128), F32),
            pltpu.VMEM((8, 8, group), F32),
            pltpu.VMEM((4, 8, group), F32),
            pltpu.VMEM((7, 8, group), F32),
            pltpu.VMEM((17, 8, 128), F32),
            dma((9,)),
            dma, dma,
            dma((4,)), dma((4,)),
            dma((3,)), dma((3,)),
            dma, dma,
            dma, dma,
            dma((3,)), dma((3,)),
            dma((4,)), dma((4,)),
            dma((4,)), dma((4,)),
            dma, dma,
        ],
        compiler_params=pltpu.CompilerParams(
            collective_id=0, has_side_effects=True, vmem_limit_bytes=48 * 1024 * 1024
        ),
        name="serve_and_count",
    )(head_ids, rel_ids, thresholds, entity_table, relations, thr_idx.reshape(16, 128))
    serving, fraction = pl.pallas_call(
        write_out,
        out_shape=(
            jax.ShapeDtypeStruct((slab, ents * n_dim), F32),
            jax.ShapeDtypeStruct((16,), F32),
        ),
        in_specs=[vmem, vmem],
        out_specs=(hbm, vmem),
        scratch_shapes=[dma((8,))],
        compiler_params=pltpu.CompilerParams(vmem_limit_bytes=1024 * 1024),
        name="write_out",
    )(landed, share)
    return serving.T, fraction


def solution(mesh):
    placed = (P(("rows", "dim"), None), P(), P(), P(), P(), P())
    return jax.shard_map(
        shards,
        mesh=mesh,
        in_specs=placed,
        out_specs=(P("rows", "dim"), P(("rows", "dim"))),
        check_vma=False,
    )
```

```python
import functools

import jax
import jax.numpy as jnp
from jax import lax
from jax.experimental import pallas as pl
from jax.experimental.pallas import tpu as pltpu
from jax.sharding import PartitionSpec as P

MESH = pl.DeviceIdType.MESH
F32 = jnp.float32
sharpness = 2.0

PLANE = [(a, b, z) for a in range(2) for b in range(2) for z in range(4)][1:]
SLABS = [(0, 1, 2), (0, 0, 2), (0, 1, 1), (0, 1, 3), (0, 1, 0), (0, 0, 1), (0, 0, 3)]
COUNTS = [1152, 256, 256, 896, 128, 128, 256, 128, 128, 256, 128, 128, 256]
WAVES = [(sum(COUNTS[:k]), COUNTS[k]) for k in range(len(COUNTS))]


def kernel(
    total_ents, head_ids_in, rel_ids_in, thresholds_in, table, relations, thr_idx_in,
    serving, share,
    head_ids, rel_ids, thresholds, thr_idx,
    tab, tab_t, ent, rel, theirs, mine, pair_in, x_in, plane_in, rel_rows, query_rows, queries,
    level, totals, pair_tot, x_tot, plane_tot,
    load_sem, slab_send, slab_recv, pair_send, pair_recv, x_send, x_recv,
    plane_send, plane_recv, gath_send, gath_recv, xg_send, xg_recv, pg_send, pg_recv,
    tot_send, tot_recv, last_send, last_recv,
):
    r, d = lax.axis_index("rows"), lax.axis_index("dim")
    x, y_lo, core = r // 4, (r // 2) % 2, r % 2
    y_hi, z = d // 4, d % 4
    ents = table.shape[0]
    width = table.shape[1]
    group = x_in.shape[1]
    slab = serving.shape[0]

    def at_plane(off):
        a, b, dz = off
        row = x * 4 + ((y_lo + a) % 2) * 2 + core
        return row, ((y_hi + b) % 2) * 4 + (z + dz) % 4

    def at_x(k):
        return ((x + k) % 4) * 4 + y_lo * 2 + core, d

    partner = (x * 4 + y_lo * 2 + (1 - core), d)

    def send(src, dst, s, t, peer):
        copy = pltpu.make_async_remote_copy(
            src_ref=src, dst_ref=dst, send_sem=s, recv_sem=t, device_id=peer, device_id_type=MESH
        )
        copy.start()
        return copy

    def all_of(src, dst, s, t):
        return pltpu.make_async_remote_copy(
            src_ref=src, dst_ref=dst, send_sem=s, recv_sem=t, device_id=partner, device_id_type=MESH
        )

    cuts = [0, COUNTS[0], 2048, 3072, ents]
    loads = []
    for k in range(4):
        span = pl.ds(cuts[k], cuts[k + 1] - cuts[k])
        loads.append(pltpu.make_async_copy(table.at[span], tab.at[span], load_sem.at[k]))
        loads[-1].start()
    small = []
    for i, (src, dst) in enumerate(
        ((head_ids_in, head_ids), (rel_ids_in, rel_ids), (thresholds_in, thresholds), (thr_idx_in, thr_idx), (relations, rel))
    ):
        small.append(pltpu.make_async_copy(src, dst, load_sem.at[4 + i]))
        small[-1].start()
    barrier = pltpu.get_barrier_semaphore()
    peers = [at_plane(off) for off in PLANE] + [at_x(k) for k in (1, 2, 3)] + [partner]
    for peer in peers:
        pl.semaphore_signal(barrier, inc=1, device_id=peer, device_id_type=MESH)

    def transpose_rows(first, count):
        @pl.loop(0, count // 128)
        def _(i):
            span = pl.ds(pl.multiple_of(first + i * 128, 128), 128)
            tab_t[:, span] = tab[span, :].T

    def start_wave(w):
        first, count = WAVES[w]
        span = pl.ds(first, count)
        here = pl.ds(pl.multiple_of(d * ents + first, 128), count)
        for off in SLABS:
            row, col = at_plane(off)
            rows = pl.ds(pl.multiple_of(col * slab, 8), slab)
            send(tab_t.at[rows, span], serving.at[:, here], slab_send, slab_recv, (row, col))
        rows = pl.ds(pl.multiple_of(d * slab, 8), slab)
        serving[:, here] = tab_t[rows, span]

    loads[0].wait()
    transpose_rows(*WAVES[0])
    pl.semaphore_wait(barrier, len(peers))
    start_wave(0)
    for k in range(1, 4):
        loads[k].wait()
    small[0].wait()

    start = (r * lax.axis_size("dim") + d) * ents
    tab[pl.ds(ents, 8), :] = jnp.zeros((8, width), F32)

    def pick(out, half, k):
        for part in range(2):
            base = k * 512 + part * 256 + half * 128

            @pl.loop(0, 16)
            def _(i):
                rows = []
                for j in range(8):
                    local = (head_ids[base + i * 8 + j] - start).astype(jnp.uint32)
                    row = jnp.minimum(local, jnp.uint32(ents)).astype(jnp.int32)
                    rows.append(tab[pl.ds(row, 1), :])
                span = pl.ds(pl.multiple_of(part * 128 + i * 8, 8), 8)
                out[k, span, :] = jnp.concatenate(rows, axis=0)

    order = [(x + 2) % 4, (x + 1) % 4, (x + 3) % 4, x]
    copies, x_copies = [], {}

    def sum_pair(n, k):
        copies[n].wait_recv()
        mine[order[n]] += pair_in[order[n]]
        if k:
            x_copies[k] = send(mine.at[order[n]], x_in.at[k - 1], x_send.at[k - 1], x_recv.at[k - 1], at_x(k))

    for n, k in enumerate((2, 1, 3, 0)):
        pick(theirs, 1 - core, order[n])
        copies.append(send(theirs.at[order[n]], pair_in.at[order[n]], pair_send.at[n], pair_recv.at[n], partner))
        if n:
            sum_pair(n - 1, (2, 1, 3, 0)[n - 1])
        pick(mine, core, order[n])
    sum_pair(3, 0)

    transpose_rows(WAVES[0][1], ents - WAVES[0][1])

    @pl.loop(0, ents // 256)
    def _(i):
        span = pl.ds(pl.multiple_of(i * 256, 256), 256)
        ent[span, :] = tab[span, :].astype(jnp.bfloat16)

    for copy in small[1:]:
        copy.wait()
    found = jnp.zeros(level.shape, F32)
    for k in range(thresholds.shape[0]):
        found = jnp.where(thr_idx[...] == k, thresholds[k], found)
    level[...] = found
    first_q = r * 128 + d * 16
    for i in range(16):
        rel_rows[pl.ds(i, 1), :] = rel[pl.ds(rel_ids[first_q + i], 1), :]

    for k in (1, 3, 2):
        x_copies[k].wait_recv()
        mine[x] += x_in[k - 1]

    def rows_of(row, col):
        return pl.ds(pl.multiple_of(((row // 2) % 2) * 128 + col * 16, 16), 16)

    for i, off in enumerate(PLANE):
        peer = at_plane(off)
        send(mine.at[x, rows_of(*peer)], plane_in.at[i], plane_send, plane_recv, peer)
    start_wave(1)
    head = mine[x, rows_of(r, d)]
    all_of(mine.at[x, pl.ds(0, 240)], plane_in, plane_send, plane_recv).wait_recv()
    for i in range(15):
        head += plane_in[i]

    query_rows[...] = (head * rel_rows[...]).astype(jnp.bfloat16).astype(F32)
    own_group = core * 4 + x
    for off in PLANE:
        send(query_rows, queries.at[own_group, rows_of(r, d)], gath_send, gath_recv, at_plane(off))
    start_wave(2)
    queries[own_group, rows_of(r, d)] = query_rows[...]
    gathered = all_of(mine.at[x, pl.ds(0, 240)], queries.at[own_group, pl.ds(0, 240)], gath_send, gath_recv)
    gathered.wait_recv()

    xg_copies = {}

    def gather_x(k):
        xg_copies[k] = send(
            queries.at[own_group], queries.at[own_group], xg_send.at[k - 1], xg_recv.at[k - 1], at_x(k)
        )

    gather_x(1)
    gather_x(3)
    start_wave(3)
    tile = 512

    def count(half, k):
        g = half * 4 + k
        low = queries[g].astype(jnp.bfloat16)
        lev = jnp.concatenate(
            [level[pl.ds(k * 4 + half, 1), :], level[pl.ds(k * 4 + 2 + half, 1), :]], axis=1
        )

        def step(i, acc):
            rows = ent[pl.ds(pl.multiple_of(i * tile, tile), tile), :]
            score = lax.dot_general(rows, low, (((1,), (1,)), ((), ())), preferred_element_type=F32)
            soft = 1.0 / (1.0 + jnp.exp(sharpness * (lev - score)))
            return acc + jnp.sum(soft.reshape(tile // 8, 8, group), axis=0)

        totals[g] = lax.fori_loop(0, ents // tile, step, jnp.zeros((8, group), F32))

    pg_copies = []

    def pass_on(n, k):
        g = core * 4 + (x + 4 - k) % 4
        pg_copies.append(send(queries.at[g], queries.at[g], pg_send.at[n], pg_recv.at[n], partner))

    def both(n, k):
        from_x = (x + 4 - k) % 4
        count(core, from_x)
        start_wave(4 + 2 * n)
        pg_copies[n].wait_recv()
        count(1 - core, from_x)
        start_wave(5 + 2 * n)

    pass_on(0, 0)
    both(0, 0)
    xg_copies[1].wait_recv()
    xg_copies[3].wait_recv()
    gather_x(2)
    pass_on(1, 1)
    pass_on(2, 3)
    both(1, 1)
    both(2, 3)
    xg_copies[2].wait_recv()
    pass_on(3, 2)
    both(3, 2)

    for copy in copies + list(x_copies.values()) + list(xg_copies.values()) + pg_copies:
        copy.wait_send()
    all_of(mine.at[x, pl.ds(0, 240)], plane_in, plane_send, plane_recv).wait_send()
    gathered.wait_send()

    other = pl.ds((1 - core) * 4, 4)
    half = send(totals.at[other], pair_tot, tot_send.at[0], tot_recv.at[0], partner)
    half.wait_recv()
    x_tots = {}
    for k in (0, 1, 2, 3):
        to = (x + k) % 4
        x_tot[k] = totals[core * 4 + to] + pair_tot[to]
        if k:
            x_tots[k] = send(x_tot.at[k], x_tot.at[3 + k], tot_send.at[k], tot_recv.at[k], at_x(k))
    sums = x_tot[0]
    for k in (1, 2, 3):
        x_tots[k].wait_recv()
        sums += x_tot[3 + k]
    plane_tot[0] = sums[:, :128]
    plane_tot[1] = sums[:, 128:]
    for i, off in enumerate(PLANE):
        row, col = at_plane(off)
        send(plane_tot.at[(row // 2) % 2], plane_tot.at[2 + i], last_send, last_recv, (row, col))
    start_wave(12)
    whole = plane_tot[y_lo]
    last = all_of(plane_tot.at[pl.ds(0, 15)], plane_tot.at[pl.ds(2, 15)], last_send, last_recv)
    last.wait_recv()
    half.wait_send()
    for k in (1, 2, 3):
        x_tots[k].wait_send()
    for i in range(15):
        whole += plane_tot[2 + i]
    whole = jnp.sum(whole, axis=0, keepdims=True) * (1.0 / total_ents)
    share[...] = pltpu.roll(jnp.broadcast_to(whole, (8, 128)), (128 - d * 16) % 128, 1)

    slabs = all_of(tab_t.at[pl.ds(0, 7 * slab)], serving.at[:, pl.ds(0, 7 * ents)], slab_send, slab_recv)
    slabs.wait_recv()
    slabs.wait_send()
    last.wait_send()


def write_out(landed, share, serving, fraction, sems):
    copies = []
    for i in range(8):
        rows = pl.ds(i * (landed.shape[0] // 8), landed.shape[0] // 8)
        copies.append(pltpu.make_async_copy(landed.at[rows], serving.at[rows], sems.at[i]))
        copies[-1].start()
    fraction[...] = share[0, :16]
    for copy in copies:
        copy.wait()


def shards(entity_table, relations, thresholds, head_ids, rel_ids, thr_idx):
    ents, width = entity_table.shape
    n_rows, n_dim = lax.axis_size("rows"), lax.axis_size("dim")
    total_ents = ents * n_rows * n_dim
    slab = width // n_dim
    group = 256
    hbm = pl.BlockSpec(memory_space=pl.ANY)
    vmem = pl.BlockSpec(memory_space=pltpu.VMEM)
    dma = pltpu.SemaphoreType.DMA
    landed, share = pl.pallas_call(
        functools.partial(kernel, total_ents),
        out_shape=(
            pltpu.VMEM((slab, ents * n_dim), F32),
            pltpu.VMEM((8, 128), F32),
        ),
        in_specs=[hbm] * 6,
        out_specs=(vmem, vmem),
        scratch_shapes=[
            pltpu.SMEM(head_ids.shape, jnp.int32),
            pltpu.SMEM(rel_ids.shape, jnp.int32),
            pltpu.SMEM(thresholds.shape, F32),
            pltpu.VMEM((16, 128), jnp.int32),
            pltpu.VMEM((ents + 8, width), F32),
            pltpu.VMEM((width, ents), F32),
            pltpu.VMEM((ents, width), jnp.bfloat16),
            pltpu.VMEM(relations.shape, F32),
            pltpu.VMEM((4, group, width), F32),
            pltpu.VMEM((4, group, width), F32),
            pltpu.VMEM((4, group, width), F32),
            pltpu.VMEM((3, group, width), F32),
            pltpu.VMEM((15, 16, width), F32),
            pltpu.VMEM((16, width), F32),
            pltpu.VMEM((16, width), F32),
            pltpu.VMEM((8, group, width), F32),
            pltpu.VMEM((16, 128), F32),
            pltpu.VMEM((8, 8, group), F32),
            pltpu.VMEM((4, 8, group), F32),
            pltpu.VMEM((7, 8, group), F32),
            pltpu.VMEM((17, 8, 128), F32),
            dma((9,)),
            dma, dma,
            dma((4,)), dma((4,)),
            dma((3,)), dma((3,)),
            dma, dma,
            dma, dma,
            dma((3,)), dma((3,)),
            dma((4,)), dma((4,)),
            dma((4,)), dma((4,)),
            dma, dma,
        ],
        compiler_params=pltpu.CompilerParams(
            collective_id=0, has_side_effects=True, vmem_limit_bytes=48 * 1024 * 1024
        ),
        name="serve_and_count",
    )(head_ids, rel_ids, thresholds, entity_table, relations, thr_idx.reshape(16, 128))
    serving, fraction = pl.pallas_call(
        write_out,
        out_shape=(
            jax.ShapeDtypeStruct((slab, ents * n_dim), F32),
            jax.ShapeDtypeStruct((16,), F32),
        ),
        in_specs=[vmem, vmem],
        out_specs=(hbm, vmem),
        scratch_shapes=[dma((8,))],
        compiler_params=pltpu.CompilerParams(vmem_limit_bytes=1024 * 1024),
        name="write_out",
    )(landed, share)
    return serving.T, fraction


def solution(mesh):
    placed = (P(("rows", "dim"), None), P(), P(), P(), P(), P())
    return jax.shard_map(
        shards,
        mesh=mesh,
        in_specs=placed,
        out_specs=(P("rows", "dim"), P(("rows", "dim"))),
        check_vma=False,
    )
```

```python
import functools

import jax
import jax.numpy as jnp
from jax import lax
from jax.experimental import pallas as pl
from jax.experimental.pallas import tpu as pltpu
from jax.sharding import PartitionSpec as P

MESH = pl.DeviceIdType.MESH
F32 = jnp.float32
sharpness = 2.0

PLANE = [(a, b, z) for a in range(2) for b in range(2) for z in range(4)][1:]
SLABS = [(0, 1, 2), (0, 0, 2), (0, 1, 1), (0, 1, 3), (0, 1, 0), (0, 0, 1), (0, 0, 3)]
COUNTS = [1152, 256, 256, 896, 128, 128, 256, 128, 128, 256, 128, 128, 256]
WAVES = [(sum(COUNTS[:k]), COUNTS[k]) for k in range(len(COUNTS))]


def kernel(
    total_ents, head_ids_in, rel_ids_in, thresholds_in, table, relations, thr_idx_in,
    serving, share,
    head_ids, rel_ids, thresholds, thr_idx,
    tab, tab_t, ent, rel, theirs, mine, pair_in, x_in, plane_in, rel_rows, query_rows, queries,
    level, totals, pair_tot, x_tot, plane_tot,
    load_sem, slab_send, slab_recv, pair_send, pair_recv, x_send, x_recv,
    plane_send, plane_recv, gath_send, gath_recv, xg_send, xg_recv, pg_send, pg_recv,
    tot_send, tot_recv, last_send, last_recv,
):
    r, d = lax.axis_index("rows"), lax.axis_index("dim")
    x, y_lo, core = r // 4, (r // 2) % 2, r % 2
    y_hi, z = d // 4, d % 4
    ents = table.shape[0]
    width = table.shape[1]
    group = x_in.shape[1]
    slab = serving.shape[0]

    def at_plane(off):
        a, b, dz = off
        row = x * 4 + ((y_lo + a) % 2) * 2 + core
        return row, ((y_hi + b) % 2) * 4 + (z + dz) % 4

    def at_x(k):
        return ((x + k) % 4) * 4 + y_lo * 2 + core, d

    partner = (x * 4 + y_lo * 2 + (1 - core), d)

    def send(src, dst, s, t, peer):
        copy = pltpu.make_async_remote_copy(
            src_ref=src, dst_ref=dst, send_sem=s, recv_sem=t, device_id=peer, device_id_type=MESH
        )
        copy.start()
        return copy

    def all_of(src, dst, s, t):
        return pltpu.make_async_remote_copy(
            src_ref=src, dst_ref=dst, send_sem=s, recv_sem=t, device_id=partner, device_id_type=MESH
        )

    cuts = [0, 512, COUNTS[0], 2560, ents]
    loads = []
    for k in range(4):
        span = pl.ds(cuts[k], cuts[k + 1] - cuts[k])
        loads.append(pltpu.make_async_copy(table.at[span], tab.at[span], load_sem.at[k]))
        loads[-1].start()
    small = []
    for i, (src, dst) in enumerate(
        ((head_ids_in, head_ids), (rel_ids_in, rel_ids), (thresholds_in, thresholds), (thr_idx_in, thr_idx), (relations, rel))
    ):
        small.append(pltpu.make_async_copy(src, dst, load_sem.at[4 + i]))
        small[-1].start()
    barrier = pltpu.get_barrier_semaphore()
    peers = [at_plane(off) for off in PLANE] + [at_x(k) for k in (1, 2, 3)] + [partner]
    for peer in peers:
        pl.semaphore_signal(barrier, inc=1, device_id=peer, device_id_type=MESH)

    def transpose_rows(first, count):
        @pl.loop(0, count // 128)
        def _(i):
            span = pl.ds(pl.multiple_of(first + i * 128, 128), 128)
            tab_t[:, span] = tab[span, :].T

    def start_wave(w):
        first, count = WAVES[w]
        span = pl.ds(first, count)
        here = pl.ds(pl.multiple_of(d * ents + first, 128), count)
        for off in SLABS:
            row, col = at_plane(off)
            rows = pl.ds(pl.multiple_of(col * slab, 8), slab)
            send(tab_t.at[rows, span], serving.at[:, here], slab_send, slab_recv, (row, col))
        rows = pl.ds(pl.multiple_of(d * slab, 8), slab)
        serving[:, here] = tab_t[rows, span]

    loads[0].wait()
    transpose_rows(0, cuts[1])
    loads[1].wait()
    transpose_rows(cuts[1], cuts[2] - cuts[1])
    pl.semaphore_wait(barrier, len(peers))
    start_wave(0)
    for k in range(2, 4):
        loads[k].wait()
    small[0].wait()

    start = (r * lax.axis_size("dim") + d) * ents
    tab[pl.ds(ents, 8), :] = jnp.zeros((8, width), F32)

    def pick(out, half, k):
        for part in range(2):
            base = k * 512 + part * 256 + half * 128

            @pl.loop(0, 16)
            def _(i):
                rows = []
                for j in range(8):
                    local = (head_ids[base + i * 8 + j] - start).astype(jnp.uint32)
                    row = jnp.minimum(local, jnp.uint32(ents)).astype(jnp.int32)
                    rows.append(tab[pl.ds(row, 1), :])
                span = pl.ds(pl.multiple_of(part * 128 + i * 8, 8), 8)
                out[k, span, :] = jnp.concatenate(rows, axis=0)

    order = [(x + 2) % 4, (x + 1) % 4, (x + 3) % 4, x]
    copies, x_copies = [], {}

    def sum_pair(n, k):
        copies[n].wait_recv()
        mine[order[n]] += pair_in[order[n]]
        if k:
            x_copies[k] = send(mine.at[order[n]], x_in.at[k - 1], x_send.at[k - 1], x_recv.at[k - 1], at_x(k))

    for n, k in enumerate((2, 1, 3, 0)):
        pick(theirs, 1 - core, order[n])
        copies.append(send(theirs.at[order[n]], pair_in.at[order[n]], pair_send.at[n], pair_recv.at[n], partner))
        if n:
            sum_pair(n - 1, (2, 1, 3, 0)[n - 1])
        pick(mine, core, order[n])
    sum_pair(3, 0)

    transpose_rows(WAVES[0][1], ents - WAVES[0][1])

    @pl.loop(0, ents // 256)
    def _(i):
        span = pl.ds(pl.multiple_of(i * 256, 256), 256)
        ent[span, :] = tab[span, :].astype(jnp.bfloat16)

    for copy in small[1:]:
        copy.wait()
    found = jnp.zeros(level.shape, F32)
    for k in range(thresholds.shape[0]):
        found = jnp.where(thr_idx[...] == k, thresholds[k], found)
    level[...] = found
    first_q = r * 128 + d * 16
    for i in range(16):
        rel_rows[pl.ds(i, 1), :] = rel[pl.ds(rel_ids[first_q + i], 1), :]

    for k in (1, 3, 2):
        x_copies[k].wait_recv()
        mine[x] += x_in[k - 1]

    def rows_of(row, col):
        return pl.ds(pl.multiple_of(((row // 2) % 2) * 128 + col * 16, 16), 16)

    for i, off in enumerate(PLANE):
        peer = at_plane(off)
        send(mine.at[x, rows_of(*peer)], plane_in.at[i], plane_send, plane_recv, peer)
    start_wave(1)
    head = mine[x, rows_of(r, d)]
    all_of(mine.at[x, pl.ds(0, 240)], plane_in, plane_send, plane_recv).wait_recv()
    for i in range(15):
        head += plane_in[i]

    query_rows[...] = (head * rel_rows[...]).astype(jnp.bfloat16).astype(F32)
    own_group = core * 4 + x
    for off in PLANE:
        send(query_rows, queries.at[own_group, rows_of(r, d)], gath_send, gath_recv, at_plane(off))
    start_wave(2)
    queries[own_group, rows_of(r, d)] = query_rows[...]
    gathered = all_of(mine.at[x, pl.ds(0, 240)], queries.at[own_group, pl.ds(0, 240)], gath_send, gath_recv)
    gathered.wait_recv()

    xg_copies = {}

    def gather_x(k):
        xg_copies[k] = send(
            queries.at[own_group], queries.at[own_group], xg_send.at[k - 1], xg_recv.at[k - 1], at_x(k)
        )

    gather_x(1)
    gather_x(3)
    start_wave(3)
    tile = 512

    def count(half, k):
        g = half * 4 + k
        low = queries[g].astype(jnp.bfloat16)
        lev = jnp.concatenate(
            [level[pl.ds(k * 4 + half, 1), :], level[pl.ds(k * 4 + 2 + half, 1), :]], axis=1
        )

        def step(i, acc):
            rows = ent[pl.ds(pl.multiple_of(i * tile, tile), tile), :]
            score = lax.dot_general(rows, low, (((1,), (1,)), ((), ())), preferred_element_type=F32)
            soft = 1.0 / (1.0 + jnp.exp(sharpness * (lev - score)))
            return acc + jnp.sum(soft.reshape(tile // 8, 8, group), axis=0)

        totals[g] = lax.fori_loop(0, ents // tile, step, jnp.zeros((8, group), F32))

    pg_copies = []

    def pass_on(n, k):
        g = core * 4 + (x + 4 - k) % 4
        pg_copies.append(send(queries.at[g], queries.at[g], pg_send.at[n], pg_recv.at[n], partner))

    def both(n, k):
        from_x = (x + 4 - k) % 4
        count(core, from_x)
        start_wave(4 + 2 * n)
        pg_copies[n].wait_recv()
        count(1 - core, from_x)
        start_wave(5 + 2 * n)

    pass_on(0, 0)
    both(0, 0)
    xg_copies[1].wait_recv()
    xg_copies[3].wait_recv()
    gather_x(2)
    pass_on(1, 1)
    pass_on(2, 3)
    both(1, 1)
    both(2, 3)
    xg_copies[2].wait_recv()
    pass_on(3, 2)
    both(3, 2)

    for copy in copies + list(x_copies.values()) + list(xg_copies.values()) + pg_copies:
        copy.wait_send()
    all_of(mine.at[x, pl.ds(0, 240)], plane_in, plane_send, plane_recv).wait_send()
    gathered.wait_send()

    other = pl.ds((1 - core) * 4, 4)
    half = send(totals.at[other], pair_tot, tot_send.at[0], tot_recv.at[0], partner)
    half.wait_recv()
    x_tots = {}
    for k in (0, 1, 2, 3):
        to = (x + k) % 4
        x_tot[k] = totals[core * 4 + to] + pair_tot[to]
        if k:
            x_tots[k] = send(x_tot.at[k], x_tot.at[3 + k], tot_send.at[k], tot_recv.at[k], at_x(k))
    sums = x_tot[0]
    for k in (1, 2, 3):
        x_tots[k].wait_recv()
        sums += x_tot[3 + k]
    plane_tot[0] = sums[:, :128]
    plane_tot[1] = sums[:, 128:]
    for i, off in enumerate(PLANE):
        row, col = at_plane(off)
        send(plane_tot.at[(row // 2) % 2], plane_tot.at[2 + i], last_send, last_recv, (row, col))
    start_wave(12)
    whole = plane_tot[y_lo]
    last = all_of(plane_tot.at[pl.ds(0, 15)], plane_tot.at[pl.ds(2, 15)], last_send, last_recv)
    last.wait_recv()
    half.wait_send()
    for k in (1, 2, 3):
        x_tots[k].wait_send()
    for i in range(15):
        whole += plane_tot[2 + i]
    whole = jnp.sum(whole, axis=0, keepdims=True) * (1.0 / total_ents)
    share[...] = pltpu.roll(jnp.broadcast_to(whole, (8, 128)), (128 - d * 16) % 128, 1)

    slabs = all_of(tab_t.at[pl.ds(0, 7 * slab)], serving.at[:, pl.ds(0, 7 * ents)], slab_send, slab_recv)
    slabs.wait_recv()
    slabs.wait_send()
    last.wait_send()


def write_out(landed, share, serving, fraction, sems):
    copies = []
    for i in range(8):
        rows = pl.ds(i * (landed.shape[0] // 8), landed.shape[0] // 8)
        copies.append(pltpu.make_async_copy(landed.at[rows], serving.at[rows], sems.at[i]))
        copies[-1].start()
    fraction[...] = share[0, :16]
    for copy in copies:
        copy.wait()


def shards(entity_table, relations, thresholds, head_ids, rel_ids, thr_idx):
    ents, width = entity_table.shape
    n_rows, n_dim = lax.axis_size("rows"), lax.axis_size("dim")
    total_ents = ents * n_rows * n_dim
    slab = width // n_dim
    group = 256
    hbm = pl.BlockSpec(memory_space=pl.ANY)
    vmem = pl.BlockSpec(memory_space=pltpu.VMEM)
    dma = pltpu.SemaphoreType.DMA
    landed, share = pl.pallas_call(
        functools.partial(kernel, total_ents),
        out_shape=(
            pltpu.VMEM((slab, ents * n_dim), F32),
            pltpu.VMEM((8, 128), F32),
        ),
        in_specs=[hbm] * 6,
        out_specs=(vmem, vmem),
        scratch_shapes=[
            pltpu.SMEM(head_ids.shape, jnp.int32),
            pltpu.SMEM(rel_ids.shape, jnp.int32),
            pltpu.SMEM(thresholds.shape, F32),
            pltpu.VMEM((16, 128), jnp.int32),
            pltpu.VMEM((ents + 8, width), F32),
            pltpu.VMEM((width, ents), F32),
            pltpu.VMEM((ents, width), jnp.bfloat16),
            pltpu.VMEM(relations.shape, F32),
            pltpu.VMEM((4, group, width), F32),
            pltpu.VMEM((4, group, width), F32),
            pltpu.VMEM((4, group, width), F32),
            pltpu.VMEM((3, group, width), F32),
            pltpu.VMEM((15, 16, width), F32),
            pltpu.VMEM((16, width), F32),
            pltpu.VMEM((16, width), F32),
            pltpu.VMEM((8, group, width), F32),
            pltpu.VMEM((16, 128), F32),
            pltpu.VMEM((8, 8, group), F32),
            pltpu.VMEM((4, 8, group), F32),
            pltpu.VMEM((7, 8, group), F32),
            pltpu.VMEM((17, 8, 128), F32),
            dma((9,)),
            dma, dma,
            dma((4,)), dma((4,)),
            dma((3,)), dma((3,)),
            dma, dma,
            dma, dma,
            dma((3,)), dma((3,)),
            dma((4,)), dma((4,)),
            dma((4,)), dma((4,)),
            dma, dma,
        ],
        compiler_params=pltpu.CompilerParams(
            collective_id=0, has_side_effects=True, vmem_limit_bytes=48 * 1024 * 1024
        ),
        name="serve_and_count",
    )(head_ids, rel_ids, thresholds, entity_table, relations, thr_idx.reshape(16, 128))
    serving, fraction = pl.pallas_call(
        write_out,
        out_shape=(
            jax.ShapeDtypeStruct((slab, ents * n_dim), F32),
            jax.ShapeDtypeStruct((16,), F32),
        ),
        in_specs=[vmem, vmem],
        out_specs=(hbm, vmem),
        scratch_shapes=[dma((8,))],
        compiler_params=pltpu.CompilerParams(vmem_limit_bytes=1024 * 1024),
        name="write_out",
    )(landed, share)
    return serving.T, fraction


def solution(mesh):
    placed = (P(("rows", "dim"), None), P(), P(), P(), P(), P())
    return jax.shard_map(
        shards,
        mesh=mesh,
        in_specs=placed,
        out_specs=(P("rows", "dim"), P(("rows", "dim"))),
        check_vma=False,
    )
```
